128 devices in a mesh: groups: 4 (over x, y), seq: 32 (over z, core).
Axes of the slice: x: 2, y: 2, z: 16, core: 2. Of those that a mesh axis runs over, the one named last changes fastest.
The devices are a block of a 8x8x16 slice.
Arguments:
- queries: bfloat16 [8192, 24576], P(('groups', 'seq')), parts along dimension 0, may hold values from -500 to 500
- kv_new: bfloat16 [8192, 576], P(('groups', 'seq')), parts along dimension 0, may hold values from -6 to 6
- kv_cache: bfloat16 [4096, 576], P(('groups', 'seq')), parts along dimension 0, may hold values from -6 to 6
- kv_gain: float32 [512], replicated, may hold values from 0.5 to 2
- w_key: bfloat16 [512, 16384], P(None, 'seq'), may hold values from -0.25 to 0.25
- w_value: bfloat16 [512, 16384], P(None, 'seq'), may hold values from -0.25 to 0.25
- prefix_len: int32 [4], P('groups'), parts along dimension 0, may hold values from 256 to 1024
Outputs:
- attended: bfloat16 [8192, 16384], P(('groups', 'seq')), parts along dimension 0
The draws below stay inside these ranges and needn't reach their ends.
There are 4 independent parts, one for each index of `groups`. The reference program is written for one: setup_inputs(seed, part) draws one part's arguments, and reference() takes and returns one part's arrays. A program takes and returns all parts, laid end to end along the dimension named above; an argument that names none is the same for every part. Nothing has to cross between parts.
Inputs may be any that keep to these rules, and one draw needn't show every extreme that they name: The stretch's tokens take positions from prefix_len on.
All inputs are finite; a program needn't handle non-finite values.
Results may differ from the reference program's by a relative error of at most 0.012.
Values may be sent and summed in bfloat16 or wider, within the bound.
No kernel may reach another device: no remote copies, remote signals or barrier semaphores. Data moves between devices by JAX's collectives and lax.ppermute only.
A program may use at most 128 MiB of HBM per device.

```python
import math
import jax
import jax.numpy as jnp
from jax import lax

H = 128
NOPE = 128
ROPE = 64
LATENT = 512
VH = 128
TOKENS = 2048
CACHE = 1024


def draw_queries(key, part):
    base_key = jax.random.fold_in(jax.random.fold_in(key, 11), 0)
    values = jnp.clip(jax.random.normal(base_key, (TOKENS, H * (NOPE + ROPE)), jnp.float32), -8.0, 8.0)
    return values.astype(jnp.bfloat16)


def block_scale(rng, extent, shards, least, top_value):
    def one(position, blocks):
        draws = jax.random.uniform(jax.random.fold_in(jax.random.fold_in(rng, 6), position), (blocks,), jnp.float32, least / len(shards), top_value / len(shards))
        return jnp.repeat(jnp.exp(draws), extent[position] // blocks).reshape((-1,) + (1,) * (len(extent) - position - 1))

    loudness = one(*shards[0])
    for cut in shards[1:]:
        loudness = loudness * one(*cut)
    return loudness


def normal_values(stream_key, extent, deviation, reach, cuts=(), kind=jnp.bfloat16):
    result = deviation * jax.random.normal(stream_key, extent, jnp.float32)
    if cuts:
        result = result * block_scale(stream_key, extent, cuts, -0.22, 0.18)
    return jnp.clip(result, -reach, reach).astype(kind)


def setup_inputs(seed: int = 0, part: int = 0) -> dict:
    arg_keys = jax.random.split(jax.random.key(seed), 8)
    part_splits = jax.random.split(jax.random.fold_in(arg_keys[7], part), 8)
    return {
        "queries": draw_queries(jax.random.fold_in(jax.random.fold_in(arg_keys[7], part), 71), part),
        "kv_new": normal_values(part_splits[1], (TOKENS, LATENT + ROPE), 1.0, 6.0, ((0, 32),)),
        "kv_cache": normal_values(part_splits[2], (CACHE, LATENT + ROPE), 1.0, 6.0, ((0, 32),)),
        "kv_gain": jnp.clip(jnp.exp(jax.random.uniform(arg_keys[3], (LATENT,), jnp.float32, math.log(0.5), math.log(2.0))), 0.5, 2.0),
        "w_key": normal_values(arg_keys[4], (LATENT, H * NOPE), LATENT ** -0.5, 0.25, ((1, 32),)),
        "w_value": normal_values(arg_keys[5], (LATENT, H * VH), LATENT ** -0.5, 0.25, ((1, 32),)),
        "prefix_len": jax.random.randint(part_splits[6], (1,), CACHE // 4, CACHE + 1).astype(jnp.int32),
    }


epsilon = 1e-06

def phases_for(positions, rope_width):
    half_width = rope_width // 2
    inverse = 10000.0 ** (-(jnp.arange(half_width, dtype=jnp.float32) * 2.0) / rope_width)
    return positions.astype(jnp.float32)[:, None] * inverse[None, :]

def rotate(values, phases):
    half_width = values.shape[-1] // 2
    front_half = values[..., :half_width]
    back_half = values[..., half_width:]
    cosine = jnp.cos(phases)
    sine_part = jnp.sin(phases)
    return jnp.concatenate([front_half * cosine - back_half * sine_part, back_half * cosine + front_half * sine_part], -1)

def reference(queries, kv_new, kv_cache, kv_gain, w_key, w_value, prefix_len):
    stretch_start = prefix_len[0]
    tokens_all = queries.shape[0]
    cached_all = kv_cache.shape[0]
    positions = stretch_start + jnp.arange(tokens_all, dtype=jnp.int32)
    phases = phases_for(positions, ROPE)
    raw_latent = kv_new[:, :LATENT].astype(jnp.float32)
    inv_rms = lax.rsqrt(lax.optimization_barrier(jnp.mean(raw_latent * raw_latent, axis=1, keepdims=True)) + epsilon)
    latent_new = (raw_latent * inv_rms * kv_gain[None, :]).astype(jnp.bfloat16)
    rope_new = rotate(kv_new[:, LATENT:].astype(jnp.float32), phases).astype(jnp.bfloat16)
    keys_all = jnp.concatenate([kv_cache, jnp.concatenate([latent_new, rope_new], 1)], 0)
    latent_all = keys_all[:, :LATENT]
    key_rope = keys_all[:, LATENT:]
    query_heads = queries.reshape(tokens_all, H, NOPE + ROPE)
    query_rot = rotate(query_heads[:, :, NOPE:].astype(jnp.float32), phases[:, None, :]).astype(jnp.bfloat16)
    query_nope = jnp.transpose(query_heads[:, :, :NOPE], (1, 0, 2))
    query_rot = jnp.transpose(query_rot, (1, 0, 2))
    key_maps = jnp.transpose(w_key.reshape(LATENT, H, NOPE), (1, 0, 2))
    value_maps = jnp.transpose(w_value.reshape(LATENT, H, VH), (1, 0, 2))
    key_index = jnp.arange(cached_all + tokens_all, dtype=jnp.int32)[None, :]
    row_index = jnp.arange(tokens_all, dtype=jnp.int32)[:, None]
    live_mask = jnp.where(key_index < cached_all, key_index < stretch_start, key_index - cached_all <= row_index)
    score_scale = 1.0 / math.sqrt(NOPE + ROPE)

    def one_head(operands):
        head_nope, head_rot, key_map, value_map = operands
        key_nope = jnp.dot(latent_all, key_map, preferred_element_type=jnp.float32).astype(jnp.bfloat16)
        value_rows = jnp.dot(latent_all, value_map, preferred_element_type=jnp.float32).astype(jnp.bfloat16)
        scores = jnp.dot(head_nope, key_nope.T, preferred_element_type=jnp.float32)
        scores = scores + jnp.dot(head_rot, key_rope.T, preferred_element_type=jnp.float32)
        scores = jnp.where(live_mask, scores * score_scale, -1e+30)
        top_score = lax.optimization_barrier(jnp.max(scores, axis=1, keepdims=True))
        exp_scores = jnp.exp(scores - top_score)
        weights = (exp_scores / lax.optimization_barrier(jnp.sum(exp_scores, axis=1, keepdims=True))).astype(jnp.bfloat16)
        return jnp.dot(weights, value_rows, preferred_element_type=jnp.float32).astype(jnp.bfloat16)
    outputs = lax.map(one_head, (query_nope, query_rot, key_maps, value_maps))
    return jnp.transpose(outputs, (1, 0, 2)).reshape(tokens_all, H * VH)
```

```python
import functools
import math

import jax
import jax.numpy as jnp
from jax import lax
from jax.experimental import pallas as pl
from jax.experimental.pallas import tpu as pltpu
from jax.sharding import Mesh
from jax.sharding import PartitionSpec as P

NOPE = 128
ROPE = 64
LATENT = 512
VH = 128
EPS = 1e-06
CHUNK = 1024
PART = 512
NEG = -1e30


def phases_for(positions, rope_width):
    half_width = rope_width // 2
    inverse = 10000.0 ** (-(jnp.arange(half_width, dtype=jnp.float32) * 2.0) / rope_width)
    return positions.astype(jnp.float32)[:, None] * inverse[None, :]


def rotate(values, phases):
    half_width = values.shape[-1] // 2
    front_half = values[..., :half_width]
    back_half = values[..., half_width:]
    cosine = jnp.cos(phases)
    sine_part = jnp.sin(phases)
    return jnp.concatenate(
        [front_half * cosine - back_half * sine_part, back_half * cosine + front_half * sine_part],
        -1,
    )


def pack_kernel(cols_ref, q_ref, o_ref, sem):
    width = o_ref.shape[2]
    copies = [
        pltpu.make_async_copy(
            q_ref.at[:, pl.ds(pl.multiple_of(cols_ref[u] * width, width), width)],
            o_ref.at[u],
            sem.at[u],
        )
        for u in range(o_ref.shape[0])
    ]
    for copy in copies:
        copy.start()
    for copy in copies:
        copy.wait()


def pack_queries(queries, cols, width):
    units = cols.shape[0]
    rows = queries.shape[0]
    return pl.pallas_call(
        pack_kernel,
        out_shape=jax.ShapeDtypeStruct((units, rows, width), queries.dtype),
        in_specs=[pl.BlockSpec(memory_space=pltpu.SMEM), pl.BlockSpec(memory_space=pl.ANY)],
        out_specs=pl.BlockSpec(memory_space=pltpu.VMEM),
        scratch_shapes=[pltpu.SemaphoreType.DMA((units,))],
        cost_estimate=pl.CostEstimate(
            flops=5_000_000, bytes_accessed=4 * units * rows * width, transcendentals=0
        ),
        name="pack",
    )(cols, queries)


def keys_kernel(chips, cache_dev, tok_dev, meta_ref, *refs):
    *ins, far_ref, out_ref = refs
    here, core = meta_ref[0], meta_ref[1]
    cache_all = chips * 2 * cache_dev
    rows = cache_dev + tok_dev
    out_ref[:, LATENT + ROPE :] = jnp.zeros_like(out_ref[:, LATENT + ROPE :])

    def place(block, chip, first_core):
        for part in range(2):
            seat = 2 * chip + (first_core if part == 0 else 1 - first_core)
            at = pl.multiple_of(seat * cache_dev, cache_dev)
            out_ref[pl.ds(at, cache_dev), : LATENT + ROPE] = block[
                part * rows : part * rows + cache_dev
            ]
            at = pl.multiple_of(cache_all + seat * tok_dev, tok_dev)
            out_ref[pl.ds(at, tok_dev), : LATENT + ROPE] = block[
                part * rows + cache_dev : (part + 1) * rows
            ]

    sign = jnp.where(core == 0, chips - 1, 1)
    for k, ref in enumerate(ins):
        place(ref[...], lax.rem(here + k * sign, chips), core)
    for k in range(far_ref.shape[0]):
        place(far_ref[k], lax.rem(here + (k + 1) * (chips - sign), chips), 1 - core)


def build_keys(meta, ins, far, chips, cache_dev, tok_dev):
    total = chips * 2 * (cache_dev + tok_dev)
    width = LATENT + 2 * ROPE
    vmem = pl.BlockSpec(memory_space=pltpu.VMEM)
    return pl.pallas_call(
        functools.partial(keys_kernel, chips, cache_dev, tok_dev),
        out_shape=jax.ShapeDtypeStruct((total, width), jnp.bfloat16),
        in_specs=[pl.BlockSpec(memory_space=pltpu.SMEM)] + [vmem] * (len(ins) + 1),
        out_specs=vmem,
        cost_estimate=pl.CostEstimate(
            flops=5_000_000, bytes_accessed=4 * total * width, transcendentals=0
        ),
        name="keys",
    )(meta, *ins, far)


def attend_kernel(cache_all, n_w, chain, first, meta_ref, *refs):
    q_refs, w_refs = refs[:n_w], refs[n_w : 2 * n_w]
    q_far, keys_ref, cos_ref, sin_ref = refs[2 * n_w : 4 + 2 * n_w]
    o_hbm, o_far, o_buf, o_sem, qa_ref, m_ref, l_ref, acc_ref = refs[4 + 2 * n_w + chain :]
    half, width = q_refs[0].shape
    tok = 2 * half
    per = width // (NOPE + ROPE)
    heads = n_w * per
    rows = heads * tok

    live_cache, first_own, first_far = meta_ref[0], meta_ref[1], meta_ref[2]
    new_count = meta_ref[3]
    scale = 1.0 / math.sqrt(NOPE + ROPE) * math.log2(math.e)

    def weight(start, count, h):
        u, at = divmod(h, per)
        return w_refs[u][start : start + count, at * NOPE : (at + 1) * NOPE]

    for h in range(heads):
        u, at = divmod(h, per)
        at = at * (NOPE + ROPE)
        block = jnp.concatenate(
            [q_refs[u][:, at : at + NOPE + ROPE], q_far[u, :, at : at + NOPE + ROPE]], 0
        )
        absorbed = lax.dot_general(
            weight(0, LATENT, h),
            block[:, :NOPE],
            (((1,), (1,)), ((), ())),
            preferred_element_type=jnp.float32,
        )
        rot = block[:, NOPE:].astype(jnp.float32)
        turned = jnp.concatenate([rot[:, ROPE // 2 :], rot[:, : ROPE // 2]], 1)
        rot = (rot * cos_ref[...] + turned * sin_ref[...]) * scale
        rot = jnp.concatenate([rot, jnp.zeros_like(rot)], 1).T
        qa_ref[:LATENT, h * tok : (h + 1) * tok] = (absorbed * scale).astype(jnp.bfloat16)
        qa_ref[LATENT:, h * tok : (h + 1) * tok] = rot.astype(jnp.bfloat16)

    m_ref[...] = jnp.full_like(m_ref, NEG)
    l_ref[...] = jnp.zeros_like(l_ref)
    acc_ref[...] = jnp.zeros_like(acc_ref)
    cache_chunks = (live_cache + CHUNK - 1) // CHUNK
    new_chunks = (new_count + CHUNK - 1) // CHUNK
    key = lax.broadcasted_iota(jnp.int32, (CHUNK, tok), 0)
    row = lax.broadcasted_iota(jnp.int32, (1, tok), 1)
    last = jnp.where(row < half, first_own + row, first_far + row - half) + (cache_all + 1)

    def step(t, carry):
        index = jnp.where(t < cache_chunks, t, t - cache_chunks + cache_all // CHUNK)
        base = pl.multiple_of(index * CHUNK, CHUNK)
        k = keys_ref[pl.ds(base, CHUNK), :]
        limit = jnp.where(t < cache_chunks, live_cache, last) - base
        mask = key < limit
        parts = [slice(g * PART, (g + 1) * PART) for g in range(rows // PART)]
        scores = [jnp.dot(k, qa_ref[:, part], preferred_element_type=jnp.float32) for part in parts]
        for part, s in zip(parts, scores):
            s = jnp.concatenate(
                [jnp.where(mask, s[:, i * tok : (i + 1) * tok], NEG) for i in range(PART // tok)], 1
            )
            m_old = m_ref[:1, part]
            m_new = jnp.maximum(m_old, jnp.max(s, axis=0, keepdims=True))
            alpha = jnp.exp2(m_old - m_new)
            p = jnp.exp2(s - m_new)
            l_ref[:1, part] = l_ref[:1, part] * alpha + jnp.sum(p, axis=0, keepdims=True)
            m_ref[:1, part] = m_new
            pv = lax.dot_general(k[:, :LATENT], p.astype(jnp.bfloat16), (((0,), (0,)), ((), ())), preferred_element_type=jnp.float32)
            acc_ref[:, part] = acc_ref[:, part] * alpha + pv
        return carry

    lax.fori_loop(0, cache_chunks + new_chunks, step, 0)

    stores = []
    for h in range(heads):
        u, at = divmod(h, per)
        part = slice(h * tok, (h + 1) * tok)
        mixed = (acc_ref[:, part] * (1.0 / l_ref[:1, part])).astype(jnp.bfloat16)
        out = lax.dot_general(
            mixed,
            weight(LATENT, LATENT, h),
            (((0,), (0,)), ((), ())),
            preferred_element_type=jnp.float32,
        ).astype(jnp.bfloat16)
        o_buf[u, :, at * VH : (at + 1) * VH] = out[:half]
        o_far[u, :, at * VH : (at + 1) * VH] = out[half:]
        if at == per - 1:
            column = pl.multiple_of(meta_ref[4 + first + u] * (per * VH), per * VH)
            stores.append(
                pltpu.make_async_copy(
                    o_buf.at[u], o_hbm.at[:, pl.ds(column, per * VH)], o_sem.at[u]
                )
            )
            stores[-1].start()
    for copy in stores:
        copy.wait()


def attend(meta, queries, q_far, weights, keys, cos, sin, out_own, out_far, first, slot, slots, cache_all):
    n_w = len(weights)
    half = queries.shape[0]
    width = q_far.shape[2]
    heads = width // (NOPE + ROPE)
    rows = n_w * heads * 2 * half
    total = keys.shape[0]
    one = pl.Buffered(1)
    whole = lambda a: pl.BlockSpec(a.shape, lambda u, m: (0,) * a.ndim, pipeline_mode=one)
    operands = [*[queries] * n_w, *weights, q_far, keys, cos, sin]
    in_specs = [
        *[pl.BlockSpec((half, width), lambda u, m, i=i: (0, m[4 + first + i])) for i in range(n_w)],
        *[whole(w) for w in weights],
        pl.BlockSpec((pl.Element(n_w), pl.Element(half), pl.Element(width)), lambda u, m: (first, 0, 0)),
        whole(keys),
        whole(cos),
        whole(sin),
    ]
    aliases = {}
    columns = queries.shape[1] // (NOPE + ROPE) * VH
    for value, position in ((out_own, 0), (out_far, 1)):
        if value is not None:
            aliases[1 + len(operands)] = position
            operands.append(value)
            in_specs.append(pl.BlockSpec(memory_space=pl.ANY))
    return pl.pallas_call(
        functools.partial(attend_kernel, cache_all, n_w, len(aliases), first),
        out_shape=(
            jax.ShapeDtypeStruct((half, columns), jnp.bfloat16),
            jax.ShapeDtypeStruct((slots, half, heads * VH), jnp.bfloat16),
        ),
        grid_spec=pltpu.PrefetchScalarGridSpec(
            num_scalar_prefetch=1,
            grid=(1,),
            in_specs=in_specs,
            out_specs=(
                pl.BlockSpec(memory_space=pl.ANY),
                pl.BlockSpec((pl.Element(n_w), pl.Element(half), pl.Element(heads * VH)), lambda u, m: (slot, 0, 0)),
            ),
            scratch_shapes=[
                pltpu.VMEM((n_w, half, heads * VH), jnp.bfloat16),
                pltpu.SemaphoreType.DMA((n_w,)),
                pltpu.VMEM((LATENT + 2 * ROPE, rows), jnp.bfloat16),
                pltpu.VMEM((8, rows), jnp.float32),
                pltpu.VMEM((8, rows), jnp.float32),
                pltpu.VMEM((LATENT, rows), jnp.float32),
            ],
        ),
        input_output_aliases=aliases,
        compiler_params=pltpu.CompilerParams(
            dimension_semantics=("arbitrary",), vmem_limit_bytes=40 * 1024 * 1024,
        ),
        cost_estimate=pl.CostEstimate(
            flops=rows * total * 2 * 1280,
            bytes_accessed=12_000_000,
            transcendentals=rows * total,
        ),
        name=f"attend{first}",
    )(meta, *operands)


def merge_kernel(cols_ref, far_ref, old_ref, out_ref, sem):
    width = far_ref.shape[2]
    copies = [
        pltpu.make_async_copy(
            far_ref.at[u],
            out_ref.at[:, pl.ds(pl.multiple_of(cols_ref[u] * width, width), width)],
            sem.at[u],
        )
        for u in range(far_ref.shape[0])
    ]
    for copy in copies:
        copy.start()
    for copy in copies:
        copy.wait()


def merge(cols, far, out):
    return pl.pallas_call(
        merge_kernel,
        out_shape=jax.ShapeDtypeStruct(out.shape, out.dtype),
        in_specs=[
            pl.BlockSpec(memory_space=pltpu.SMEM),
            pl.BlockSpec(memory_space=pltpu.VMEM),
            pl.BlockSpec(memory_space=pl.ANY),
        ],
        out_specs=pl.BlockSpec(memory_space=pl.ANY),
        scratch_shapes=[pltpu.SemaphoreType.DMA((far.shape[0],))],
        input_output_aliases={2: 0},
        cost_estimate=pl.CostEstimate(flops=5_000_000, bytes_accessed=4 * far.size, transcendentals=0),
        name="merge",
    )(cols, far, out)


def local(queries, kv_new, kv_cache, kv_gain, w_key, w_value, prefix_len):
    gx, gy, chips = lax.axis_size("gx"), lax.axis_size("gy"), lax.axis_size("sz")
    x, y, here, core = (lax.axis_index(a) for a in ("gx", "gy", "sz", "sc"))
    tok_dev = queries.shape[0]
    cache_dev = kv_cache.shape[0]
    heads_dev = w_key.shape[1] // NOPE
    width = heads_dev * (NOPE + ROPE)
    cache_all = 2 * chips * cache_dev
    far_steps = chips // 2
    stretch_start = prefix_len[0]

    swap = [(0, 1), (1, 0)]
    ring = []
    for i in range(chips):
        ring += [(2 * i, 2 * ((i + 1) % chips)), (2 * i + 1, 2 * ((i - 1) % chips) + 1)]
    pairs = []
    for i in range(gx):
        for j in range(gy):
            at = (i * gy + j) * 2
            pairs += [(at, ((i ^ 1) * gy + j) * 2), (at + 1, (i * gy + (j ^ 1)) * 2 + 1)]

    def across(v):
        return lax.ppermute(v, "sc", swap)

    def along(v):
        return lax.ppermute(v, ("sz", "sc"), ring)

    def beside(v):
        return lax.ppermute(v, ("gx", "gy", "sc"), pairs)

    def owners(side):
        bit = jnp.where(side == 0, x % 2, y % 2)
        turn = jnp.where(side == 0, chips - 1, 1)
        units = [2 * here + side]
        for k in range(1, far_steps):
            chip = lax.rem(here + k * turn, chips)
            units += [2 * chip + bit, 2 * chip + 1 - bit]
        units.append(2 * lax.rem(here + far_steps, chips) + side)
        return jnp.stack(units).astype(jnp.int32)

    seat = 2 * here + core
    offsets = jnp.arange(tok_dev, dtype=jnp.int32)
    positions = stretch_start + seat * tok_dev + offsets
    phases = phases_for(positions, ROPE)
    raw_latent = kv_new[:, :LATENT].astype(jnp.float32)
    inv_rms = lax.rsqrt(jnp.mean(raw_latent * raw_latent, axis=1, keepdims=True) + EPS)
    latent_new = (raw_latent * inv_rms * kv_gain[None, :]).astype(jnp.bfloat16)
    rope_new = rotate(kv_new[:, LATENT:].astype(jnp.float32), phases).astype(jnp.bfloat16)
    mine = jnp.concatenate([kv_cache, jnp.concatenate([latent_new, rope_new], 1)], 0)
    own_cols, far_cols = owners(core), owners(1 - core)
    block = jnp.concatenate([mine, across(mine)], 0)
    block, w_key, w_value, far_cols = lax.optimization_barrier((block, w_key, w_value, far_cols))
    blocks = [block]
    for _ in range(far_steps):
        blocks.append(along(blocks[-1]))
    far = across(jnp.stack(blocks[1:far_steps]))
    keys = build_keys(
        jnp.stack([here, core]).astype(jnp.int32), blocks, far, chips, cache_dev, tok_dev
    )

    q_far = across(pack_queries(queries, far_cols, width))

    w_mine = jnp.concatenate([w_key, w_value], 0)
    bit = jnp.where(core == 0, x % 2, y % 2)
    travel = jnp.where(bit == core, w_mine, across(w_mine))
    steps = []
    for k in range(1, far_steps):
        travel = along(travel)
        steps.append((travel, beside(travel)))
        if k == 1:
            travel, _ = lax.optimization_barrier((travel, blocks[-2]))
    last = along(jnp.where(bit == core, *steps[-1]))

    both = jnp.concatenate(
        [positions, stretch_start + (2 * here + 1 - core) * tok_dev + offsets]
    )
    turns = phases_for(both, ROPE)
    cos = jnp.concatenate([jnp.cos(turns)] * 2, 1)
    sin = jnp.concatenate([-jnp.sin(turns), jnp.sin(turns)], 1)
    meta = jnp.concatenate(
        [
            jnp.stack(
                [
                    stretch_start,
                    seat * tok_dev,
                    (2 * here + 1 - core) * tok_dev,
                    (here + 1) * 2 * tok_dev,
                ]
            ).astype(jnp.int32),
            own_cols,
        ]
    )
    calls = [(w_mine,)] + steps + [(last,)]
    cuts = (0, len(calls) // 2, len(calls) - 1, len(calls))
    out_own = None
    first = 0
    landed = None

    def land(out):
        start, slots, value = landed
        return merge(far_cols[start : start + slots], value, out)

    for begin, end in zip(cuts, cuts[1:]):
        slots = sum(len(c) for c in calls[begin:end])
        out_far, slot = None, 0
        for i, weights in enumerate(calls[begin:end]):
            out_own, out_far = attend(
                meta, queries, q_far, weights, keys, cos, sin,
                out_own, out_far, first, slot, slots, cache_all,
            )
            first += len(weights)
            slot += len(weights)
            if landed is not None and (i == 1 or end == len(calls)):
                out_own = land(out_own)
                landed = None
        landed = (first - slots, slots, across(out_far))
    return land(out_own)


def solution(mesh):
    groups, seq = mesh.shape["groups"], mesh.shape["seq"]
    gy = math.isqrt(groups)
    torus = Mesh(
        mesh.devices.reshape(groups // gy, gy, seq // 2, 2), ("gx", "gy", "sz", "sc")
    )
    every = ("gx", "gy", "sz", "sc")
    line = ("sz", "sc")
    placed = (
        P(every, None),
        P(every, None),
        P(every, None),
        P(),
        P(None, line),
        P(None, line),
        P(("gx", "gy")),
    )
    return jax.shard_map(
        local, mesh=torus, in_specs=placed, out_specs=P(every, None), check_vma=False
    )
```

```python
import functools
import math

import jax
import jax.numpy as jnp
from jax import lax
from jax.experimental import pallas as pl
from jax.experimental.pallas import tpu as pltpu
from jax.sharding import Mesh
from jax.sharding import PartitionSpec as P

NOPE = 128
ROPE = 64
LATENT = 512
VH = 128
EPS = 1e-06
CHUNK = 1024
PART = 512
NEG = -1e30


def phases_for(positions, rope_width):
    half_width = rope_width // 2
    inverse = 10000.0 ** (-(jnp.arange(half_width, dtype=jnp.float32) * 2.0) / rope_width)
    return positions.astype(jnp.float32)[:, None] * inverse[None, :]


def rotate(values, phases):
    half_width = values.shape[-1] // 2
    front_half = values[..., :half_width]
    back_half = values[..., half_width:]
    cosine = jnp.cos(phases)
    sine_part = jnp.sin(phases)
    return jnp.concatenate(
        [front_half * cosine - back_half * sine_part, back_half * cosine + front_half * sine_part],
        -1,
    )


def pack_kernel(cols_ref, q_ref, o_ref, sem):
    width = o_ref.shape[2]
    copies = [
        pltpu.make_async_copy(
            q_ref.at[:, pl.ds(pl.multiple_of(cols_ref[u] * width, width), width)],
            o_ref.at[u],
            sem.at[u],
        )
        for u in range(o_ref.shape[0])
    ]
    for copy in copies:
        copy.start()
    for copy in copies:
        copy.wait()


def pack_queries(queries, cols, width):
    units = cols.shape[0]
    rows = queries.shape[0]
    return pl.pallas_call(
        pack_kernel,
        out_shape=jax.ShapeDtypeStruct((units, rows, width), queries.dtype),
        in_specs=[pl.BlockSpec(memory_space=pltpu.SMEM), pl.BlockSpec(memory_space=pl.ANY)],
        out_specs=pl.BlockSpec(memory_space=pltpu.VMEM),
        scratch_shapes=[pltpu.SemaphoreType.DMA((units,))],
        cost_estimate=pl.CostEstimate(
            flops=5_000_000, bytes_accessed=4 * units * rows * width, transcendentals=0
        ),
        name="pack",
    )(cols, queries)


def keys_kernel(chips, cache_dev, tok_dev, meta_ref, *refs):
    ins, fars, out_ref = refs[: chips // 2 + 1], refs[chips // 2 + 1 : -1], refs[-1]
    here, core = meta_ref[0], meta_ref[1]
    cache_all = chips * 2 * cache_dev
    rows = cache_dev + tok_dev
    out_ref[:, LATENT + ROPE :] = jnp.zeros_like(out_ref[:, LATENT + ROPE :])

    def place(block, chip, first_core):
        for part in range(2):
            seat = 2 * chip + (first_core if part == 0 else 1 - first_core)
            at = pl.multiple_of(seat * cache_dev, cache_dev)
            out_ref[pl.ds(at, cache_dev), : LATENT + ROPE] = block[
                part * rows : part * rows + cache_dev
            ]
            at = pl.multiple_of(cache_all + seat * tok_dev, tok_dev)
            out_ref[pl.ds(at, tok_dev), : LATENT + ROPE] = block[
                part * rows + cache_dev : (part + 1) * rows
            ]

    sign = jnp.where(core == 0, chips - 1, 1)
    for k, ref in enumerate(ins):
        place(ref[...], lax.rem(here + k * sign, chips), core)
    for k, ref in enumerate(fars):
        place(ref[...], lax.rem(here + (k + 1) * (chips - sign), chips), 1 - core)


def build_keys(meta, ins, chips, cache_dev, tok_dev):
    total = chips * 2 * (cache_dev + tok_dev)
    width = LATENT + 2 * ROPE
    vmem = pl.BlockSpec(memory_space=pltpu.VMEM)
    return pl.pallas_call(
        functools.partial(keys_kernel, chips, cache_dev, tok_dev),
        out_shape=jax.ShapeDtypeStruct((total, width), jnp.bfloat16),
        in_specs=[pl.BlockSpec(memory_space=pltpu.SMEM)] + [vmem] * len(ins),
        out_specs=vmem,
        cost_estimate=pl.CostEstimate(
            flops=5_000_000, bytes_accessed=4 * total * width, transcendentals=0
        ),
        name="keys",
    )(meta, *ins)


def attend_kernel(cache_all, n_w, chain, first, meta_ref, *refs):
    w_refs = refs[:n_w]
    q_own, q_far, keys_ref, cos_ref, sin_ref = refs[n_w : 5 + n_w]
    o_hbm, o_far, o_buf, o_sem, qa_ref, m_ref, l_ref, acc_ref = refs[5 + n_w + chain :]
    half, width = q_far.shape[1:]
    tok = 2 * half
    per = width // (NOPE + ROPE)
    heads = n_w * per
    rows = heads * tok

    live_cache, first_own, first_far = meta_ref[0], meta_ref[1], meta_ref[2]
    new_count = meta_ref[3]
    scale = 1.0 / math.sqrt(NOPE + ROPE) * math.log2(math.e)

    def weight(start, count, h):
        u, at = divmod(h, per)
        return w_refs[u][start : start + count, at * NOPE : (at + 1) * NOPE]

    for h in range(heads):
        u, at = divmod(h, per)
        at = at * (NOPE + ROPE)
        if at == 0:
            column = pl.multiple_of(meta_ref[4 + first + u] * width, width)
            unit = jnp.concatenate([q_own[:, pl.ds(column, width)], q_far[first + u]], 0)
        block = unit[:, at : at + NOPE + ROPE]
        absorbed = lax.dot_general(
            weight(0, LATENT, h),
            block[:, :NOPE],
            (((1,), (1,)), ((), ())),
            preferred_element_type=jnp.float32,
        )
        rot = block[:, NOPE:].astype(jnp.float32)
        turned = jnp.concatenate([rot[:, ROPE // 2 :], rot[:, : ROPE // 2]], 1)
        rot = (rot * cos_ref[...] + turned * sin_ref[...]) * scale
        rot = jnp.concatenate([rot, jnp.zeros_like(rot)], 1).T
        qa_ref[:LATENT, h * tok : (h + 1) * tok] = (absorbed * scale).astype(jnp.bfloat16)
        qa_ref[LATENT:, h * tok : (h + 1) * tok] = rot.astype(jnp.bfloat16)

    m_ref[...] = jnp.full_like(m_ref, NEG)
    l_ref[...] = jnp.zeros_like(l_ref)
    acc_ref[...] = jnp.zeros_like(acc_ref)
    cache_chunks = (live_cache + CHUNK - 1) // CHUNK
    new_chunks = (new_count + CHUNK - 1) // CHUNK
    key = lax.broadcasted_iota(jnp.int32, (CHUNK, tok), 0)
    row = lax.broadcasted_iota(jnp.int32, (1, tok), 1)
    last = jnp.where(row < half, first_own + row, first_far + row - half) + (cache_all + 1)

    def step(t, carry):
        index = jnp.where(t < cache_chunks, t, t - cache_chunks + cache_all // CHUNK)
        base = pl.multiple_of(index * CHUNK, CHUNK)
        k = keys_ref[pl.ds(base, CHUNK), :]
        limit = jnp.where(t < cache_chunks, live_cache, last) - base
        mask = key < limit
        parts = [slice(g * PART, (g + 1) * PART) for g in range(rows // PART)]
        scores = [jnp.dot(k, qa_ref[:, part], preferred_element_type=jnp.float32) for part in parts]
        for part, s in zip(parts, scores):
            s = jnp.concatenate(
                [jnp.where(mask, s[:, i * tok : (i + 1) * tok], NEG) for i in range(PART // tok)], 1
            )
            m_old = m_ref[:1, part]
            m_new = jnp.maximum(m_old, jnp.max(s, axis=0, keepdims=True))
            alpha = jnp.exp2(m_old - m_new)
            p = jnp.exp2(s - m_new)
            l_ref[:1, part] = l_ref[:1, part] * alpha + jnp.sum(p, axis=0, keepdims=True)
            m_ref[:1, part] = m_new
            pv = lax.dot_general(k[:, :LATENT], p.astype(jnp.bfloat16), (((0,), (0,)), ((), ())), preferred_element_type=jnp.float32)
            acc_ref[:, part] = acc_ref[:, part] * alpha + pv
        return carry

    lax.fori_loop(0, cache_chunks + new_chunks, step, 0)

    stores = []
    for h in range(heads):
        u, at = divmod(h, per)
        part = slice(h * tok, (h + 1) * tok)
        mixed = (acc_ref[:, part] * (1.0 / l_ref[:1, part])).astype(jnp.bfloat16)
        out = lax.dot_general(
            mixed,
            weight(LATENT, LATENT, h),
            (((0,), (0,)), ((), ())),
            preferred_element_type=jnp.float32,
        ).astype(jnp.bfloat16)
        o_buf[u, :, at * VH : (at + 1) * VH] = out[:half]
        o_far[u, :, at * VH : (at + 1) * VH] = out[half:]
        if at == per - 1:
            column = pl.multiple_of(meta_ref[4 + first + u] * (per * VH), per * VH)
            stores.append(
                pltpu.make_async_copy(
                    o_buf.at[u], o_hbm.at[:, pl.ds(column, per * VH)], o_sem.at[u]
                )
            )
            stores[-1].start()
    for copy in stores:
        copy.wait()


def attend(meta, queries, q_far, weights, keys, cos, sin, out_own, out_far, first, slot, slots, cache_all):
    n_w = len(weights)
    half = queries.shape[0]
    width = q_far.shape[2]
    heads = width // (NOPE + ROPE)
    rows = n_w * heads * 2 * half
    total = keys.shape[0]
    vmem = pl.BlockSpec(memory_space=pltpu.VMEM)
    operands = [*weights, queries, q_far, keys, cos, sin]
    in_specs = [vmem] * len(operands)
    aliases = {}
    columns = queries.shape[1] // (NOPE + ROPE) * VH
    for value, position in ((out_own, 0), (out_far, 1)):
        if value is not None:
            aliases[1 + len(operands)] = position
            operands.append(value)
            in_specs.append(pl.BlockSpec(memory_space=pl.ANY))
    return pl.pallas_call(
        functools.partial(attend_kernel, cache_all, n_w, len(aliases), first),
        out_shape=(
            jax.ShapeDtypeStruct((half, columns), jnp.bfloat16),
            jax.ShapeDtypeStruct((slots, half, heads * VH), jnp.bfloat16),
        ),
        grid_spec=pltpu.PrefetchScalarGridSpec(
            num_scalar_prefetch=1,
            grid=(1,),
            in_specs=in_specs,
            out_specs=(
                pl.BlockSpec(memory_space=pl.ANY),
                pl.BlockSpec((n_w, half, heads * VH), lambda u, m: (slot // n_w, 0, 0)),
            ),
            scratch_shapes=[
                pltpu.VMEM((n_w, half, heads * VH), jnp.bfloat16),
                pltpu.SemaphoreType.DMA((n_w,)),
                pltpu.VMEM((LATENT + 2 * ROPE, rows), jnp.bfloat16),
                pltpu.VMEM((8, rows), jnp.float32),
                pltpu.VMEM((8, rows), jnp.float32),
                pltpu.VMEM((LATENT, rows), jnp.float32),
            ],
        ),
        input_output_aliases=aliases,
        compiler_params=pltpu.CompilerParams(
            dimension_semantics=("arbitrary",), vmem_limit_bytes=32 * 1024 * 1024,
        ),
        cost_estimate=pl.CostEstimate(
            flops=rows * total * 2 * 1280,
            bytes_accessed=12_000_000,
            transcendentals=rows * total,
        ),
    )(meta, *operands)


def merge_kernel(starts, cols_ref, *refs):
    far_refs, out_ref, sem = refs[: len(starts)], refs[-2], refs[-1]
    copies = []
    for start, far_ref in zip(starts, far_refs):
        width = far_ref.shape[2]
        for u in range(far_ref.shape[0]):
            column = pl.multiple_of(cols_ref[start + u] * width, width)
            copies.append(
                pltpu.make_async_copy(
                    far_ref.at[u], out_ref.at[:, pl.ds(column, width)], sem.at[len(copies)]
                )
            )
    for copy in copies:
        copy.start()
    for copy in copies:
        copy.wait()


def merge(cols, landed, out):
    starts = tuple(start for start, _ in landed)
    fars = [value for _, value in landed]
    vmem = pl.BlockSpec(memory_space=pltpu.VMEM)
    return pl.pallas_call(
        functools.partial(merge_kernel, starts),
        out_shape=jax.ShapeDtypeStruct(out.shape, out.dtype),
        in_specs=[
            pl.BlockSpec(memory_space=pltpu.SMEM),
            *[vmem] * len(fars),
            pl.BlockSpec(memory_space=pl.ANY),
        ],
        out_specs=pl.BlockSpec(memory_space=pl.ANY),
        scratch_shapes=[pltpu.SemaphoreType.DMA((sum(f.shape[0] for f in fars),))],
        input_output_aliases={1 + len(fars): 0},
        cost_estimate=pl.CostEstimate(
            flops=5_000_000, bytes_accessed=4 * sum(f.size for f in fars), transcendentals=0
        ),
        name="merge",
    )(cols, *fars, out)


def local(queries, kv_new, kv_cache, kv_gain, w_key, w_value, prefix_len):
    gx, gy, chips = lax.axis_size("gx"), lax.axis_size("gy"), lax.axis_size("sz")
    x, y, here, core = (lax.axis_index(a) for a in ("gx", "gy", "sz", "sc"))
    tok_dev = queries.shape[0]
    cache_dev = kv_cache.shape[0]
    heads_dev = w_key.shape[1] // NOPE
    width = heads_dev * (NOPE + ROPE)
    cache_all = 2 * chips * cache_dev
    far_steps = chips // 2
    stretch_start = prefix_len[0]

    swap = [(0, 1), (1, 0)]
    ring = []
    for i in range(chips):
        ring += [(2 * i, 2 * ((i + 1) % chips)), (2 * i + 1, 2 * ((i - 1) % chips) + 1)]
    pairs = []
    for i in range(gx):
        for j in range(gy):
            at = (i * gy + j) * 2
            pairs += [(at, ((i ^ 1) * gy + j) * 2), (at + 1, (i * gy + (j ^ 1)) * 2 + 1)]

    def across(v):
        return lax.ppermute(v, "sc", swap)

    def along(v):
        return lax.ppermute(v, ("sz", "sc"), ring)

    def beside(v):
        return lax.ppermute(v, ("gx", "gy", "sc"), pairs)

    def owners(side):
        bit = jnp.where(side == 0, x % 2, y % 2)
        turn = jnp.where(side == 0, chips - 1, 1)
        units = [2 * here + side]
        for k in range(1, far_steps):
            chip = lax.rem(here + k * turn, chips)
            units += [2 * chip + bit, 2 * chip + 1 - bit]
        units.append(2 * lax.rem(here + far_steps, chips) + side)
        return jnp.stack(units).astype(jnp.int32)

    seat = 2 * here + core
    offsets = jnp.arange(tok_dev, dtype=jnp.int32)
    positions = stretch_start + seat * tok_dev + offsets
    phases = phases_for(positions, ROPE)
    raw_latent = kv_new[:, :LATENT].astype(jnp.float32)
    inv_rms = lax.rsqrt(jnp.mean(raw_latent * raw_latent, axis=1, keepdims=True) + EPS)
    latent_new = (raw_latent * inv_rms * kv_gain[None, :]).astype(jnp.bfloat16)
    rope_new = rotate(kv_new[:, LATENT:].astype(jnp.float32), phases).astype(jnp.bfloat16)
    mine = jnp.concatenate([kv_cache, jnp.concatenate([latent_new, rope_new], 1)], 0)
    own_cols, far_cols = owners(core), owners(1 - core)
    block = jnp.concatenate([mine, across(mine)], 0)
    block, w_key, w_value, far_cols = lax.optimization_barrier((block, w_key, w_value, far_cols))
    blocks, fars = [block], []
    for k in range(1, far_steps + 1):
        blocks.append(along(blocks[-1]))
        if k < far_steps:
            fars.append(across(blocks[k]))
    keys = build_keys(
        jnp.stack([here, core]).astype(jnp.int32), blocks + fars, chips, cache_dev, tok_dev
    )
    packed = pack_queries(queries, far_cols, width)
    q_far = across(packed)
    w_mine = jnp.concatenate([w_key, w_value], 0)
    bit = jnp.where(core == 0, x % 2, y % 2)
    travel = jnp.where(bit == core, w_mine, across(w_mine))

    both = jnp.concatenate(
        [positions, stretch_start + (2 * here + 1 - core) * tok_dev + offsets]
    )
    turns = phases_for(both, ROPE)
    cos = jnp.concatenate([jnp.cos(turns)] * 2, 1)
    sin = jnp.concatenate([-jnp.sin(turns), jnp.sin(turns)], 1)
    meta = jnp.concatenate(
        [
            jnp.stack(
                [
                    stretch_start,
                    seat * tok_dev,
                    (2 * here + 1 - core) * tok_dev,
                    (here + 1) * 2 * tok_dev,
                ]
            ).astype(jnp.int32),
            own_cols,
        ]
    )
    near = along(travel)
    aside = w_mine
    out_own, first = None, 0
    landed = []
    cuts = (0, far_steps // 2, far_steps, far_steps + 1)
    for begin, end in zip(cuts, cuts[1:]):
        sizes = [2 if k < far_steps - 1 else 1 for k in range(begin, end)]
        out_far, slot = None, 0
        for k in range(begin, end):
            if k < far_steps - 1:
                weights = (aside, near)
                aside = beside(near)
                if k < far_steps - 2:
                    near = along(near)
            elif k == far_steps - 1:
                weights = (aside,)
                near = along(jnp.where(bit == core, near, aside))
            else:
                weights = (near,)
            out_own, out_far = attend(
                meta, queries, q_far, weights, keys, cos, sin,
                out_own, out_far, first, slot, sum(sizes), cache_all,
            )
            first += len(weights)
            slot += len(weights)
            if landed and k == begin and end <= far_steps:
                out_own = merge(far_cols, landed, out_own)
                landed = []
        landed.append((first - slot, across(out_far)))
    return merge(far_cols, landed, out_own)


def solution(mesh):
    groups, seq = mesh.shape["groups"], mesh.shape["seq"]
    gy = math.isqrt(groups)
    torus = Mesh(
        mesh.devices.reshape(groups // gy, gy, seq // 2, 2), ("gx", "gy", "sz", "sc")
    )
    every = ("gx", "gy", "sz", "sc")
    line = ("sz", "sc")
    placed = (
        P(every, None),
        P(every, None),
        P(every, None),
        P(),
        P(None, line),
        P(None, line),
        P(("gx", "gy")),
    )
    return jax.shard_map(
        local, mesh=torus, in_specs=placed, out_specs=P(every, None), check_vma=False
    )
```

```python
import functools
import math

import jax
import jax.numpy as jnp
from jax import lax
from jax.experimental import pallas as pl
from jax.experimental.pallas import tpu as pltpu
from jax.sharding import Mesh
from jax.sharding import PartitionSpec as P

NOPE = 128
ROPE = 64
LATENT = 512
VH = 128
EPS = 1e-06
CHUNK = 1024
PART = 512
NEG = -1e30


def phases_for(positions, rope_width):
    half_width = rope_width // 2
    inverse = 10000.0 ** (-(jnp.arange(half_width, dtype=jnp.float32) * 2.0) / rope_width)
    return positions.astype(jnp.float32)[:, None] * inverse[None, :]


def rotate(values, phases):
    half_width = values.shape[-1] // 2
    front_half = values[..., :half_width]
    back_half = values[..., half_width:]
    cosine = jnp.cos(phases)
    sine_part = jnp.sin(phases)
    return jnp.concatenate(
        [front_half * cosine - back_half * sine_part, back_half * cosine + front_half * sine_part],
        -1,
    )


def pack_kernel(cols_ref, q_ref, o_ref, sem):
    width = o_ref.shape[2]
    copies = [
        pltpu.make_async_copy(
            q_ref.at[:, pl.ds(pl.multiple_of(cols_ref[u] * width, width), width)],
            o_ref.at[u],
            sem.at[u],
        )
        for u in range(o_ref.shape[0])
    ]
    for copy in copies:
        copy.start()
    for copy in copies:
        copy.wait()


def pack_queries(queries, cols, width):
    units = cols.shape[0]
    rows = queries.shape[0]
    return pl.pallas_call(
        pack_kernel,
        out_shape=jax.ShapeDtypeStruct((units, rows, width), queries.dtype),
        in_specs=[pl.BlockSpec(memory_space=pltpu.SMEM), pl.BlockSpec(memory_space=pl.ANY)],
        out_specs=pl.BlockSpec(memory_space=pltpu.VMEM),
        scratch_shapes=[pltpu.SemaphoreType.DMA((units,))],
        cost_estimate=pl.CostEstimate(
            flops=5_000_000, bytes_accessed=4 * units * rows * width, transcendentals=0
        ),
        compiler_params=pltpu.CompilerParams(vmem_limit_bytes=4 * 1024 * 1024),
        name="pack",
    )(cols, queries)


def keys_kernel(chips, cache_dev, tok_dev, meta_ref, *refs):
    ins, fars, out_ref = refs[: chips // 2 + 1], refs[chips // 2 + 1 : -1], refs[-1]
    here, core = meta_ref[0], meta_ref[1]
    cache_all = chips * 2 * cache_dev
    rows = cache_dev + tok_dev
    out_ref[:, LATENT + ROPE :] = jnp.zeros_like(out_ref[:, LATENT + ROPE :])

    def place(block, chip, first_core):
        for part in range(2):
            seat = 2 * chip + (first_core if part == 0 else 1 - first_core)
            at = pl.multiple_of(seat * cache_dev, cache_dev)
            out_ref[pl.ds(at, cache_dev), : LATENT + ROPE] = block[
                part * rows : part * rows + cache_dev
            ]
            at = pl.multiple_of(cache_all + seat * tok_dev, tok_dev)
            out_ref[pl.ds(at, tok_dev), : LATENT + ROPE] = block[
                part * rows + cache_dev : (part + 1) * rows
            ]

    sign = jnp.where(core == 0, chips - 1, 1)
    for k, ref in enumerate(ins):
        place(ref[...], lax.rem(here + k * sign, chips), core)
    for k, ref in enumerate(fars):
        place(ref[...], lax.rem(here + (k + 1) * (chips - sign), chips), 1 - core)


def build_keys(meta, ins, chips, cache_dev, tok_dev):
    total = chips * 2 * (cache_dev + tok_dev)
    width = LATENT + 2 * ROPE
    vmem = pl.BlockSpec(memory_space=pltpu.VMEM)
    return pl.pallas_call(
        functools.partial(keys_kernel, chips, cache_dev, tok_dev),
        out_shape=jax.ShapeDtypeStruct((total, width), jnp.bfloat16),
        in_specs=[pl.BlockSpec(memory_space=pltpu.SMEM)] + [vmem] * len(ins),
        out_specs=vmem,
        cost_estimate=pl.CostEstimate(
            flops=5_000_000, bytes_accessed=4 * total * width, transcendentals=0
        ),
        compiler_params=pltpu.CompilerParams(vmem_limit_bytes=16 * 1024 * 1024),
        name="keys",
    )(meta, *ins)


def attend_kernel(cache_all, n_w, chain, first, slot, meta_ref, *refs):
    w_refs = refs[:n_w]
    q_own, q_far, keys_ref, cos_ref, sin_ref = refs[n_w : 5 + n_w]
    o_own, o_far, qa_ref, m_ref, l_ref, acc_ref = refs[5 + n_w + chain :]
    half, width = q_far.shape[1:]
    tok = 2 * half
    per = width // (NOPE + ROPE)
    heads = n_w * per
    rows = heads * tok

    live_cache, first_own, first_far = meta_ref[0], meta_ref[1], meta_ref[2]
    new_count = meta_ref[3]
    scale = 1.0 / math.sqrt(NOPE + ROPE) * math.log2(math.e)

    def weight(start, count, h):
        u, at = divmod(h, per)
        return w_refs[u][start : start + count, at * NOPE : (at + 1) * NOPE]

    for h in range(heads):
        u, at = divmod(h, per)
        at = at * (NOPE + ROPE)
        if at == 0:
            column = pl.multiple_of(meta_ref[4 + first + u] * width, width)
            unit = jnp.concatenate([q_own[:, pl.ds(column, width)], q_far[first + u]], 0)
        block = unit[:, at : at + NOPE + ROPE]
        absorbed = lax.dot_general(
            weight(0, LATENT, h),
            block[:, :NOPE],
            (((1,), (1,)), ((), ())),
            preferred_element_type=jnp.float32,
        )
        rot = block[:, NOPE:].astype(jnp.float32)
        turned = jnp.concatenate([rot[:, ROPE // 2 :], rot[:, : ROPE // 2]], 1)
        rot = (rot * cos_ref[...] + turned * sin_ref[...]) * scale
        rot = jnp.concatenate([rot, jnp.zeros_like(rot)], 1).T
        qa_ref[:LATENT, h * tok : (h + 1) * tok] = (absorbed * scale).astype(jnp.bfloat16)
        qa_ref[LATENT:, h * tok : (h + 1) * tok] = rot.astype(jnp.bfloat16)

    m_ref[...] = jnp.full_like(m_ref, NEG)
    l_ref[...] = jnp.zeros_like(l_ref)
    acc_ref[...] = jnp.zeros_like(acc_ref)
    cache_chunks = (live_cache + CHUNK - 1) // CHUNK
    new_chunks = (new_count + CHUNK - 1) // CHUNK
    key = lax.broadcasted_iota(jnp.int32, (CHUNK, tok), 0)
    row = lax.broadcasted_iota(jnp.int32, (1, tok), 1)
    last = jnp.where(row < half, first_own + row, first_far + row - half) + (cache_all + 1)

    def step(t, carry):
        index = jnp.where(t < cache_chunks, t, t - cache_chunks + cache_all // CHUNK)
        base = pl.multiple_of(index * CHUNK, CHUNK)
        k = keys_ref[pl.ds(base, CHUNK), :]
        limit = jnp.where(t < cache_chunks, live_cache, last) - base
        mask = key < limit
        parts = [slice(g * PART, (g + 1) * PART) for g in range(rows // PART)]
        scores = [jnp.dot(k, qa_ref[:, part], preferred_element_type=jnp.float32) for part in parts]
        for part, s in zip(parts, scores):
            s = jnp.concatenate(
                [jnp.where(mask, s[:, i * tok : (i + 1) * tok], NEG) for i in range(PART // tok)], 1
            )
            m_old = m_ref[:1, part]
            m_new = jnp.maximum(m_old, jnp.max(s, axis=0, keepdims=True))
            alpha = jnp.exp2(m_old - m_new)
            p = jnp.exp2(s - m_new)
            l_ref[:1, part] = l_ref[:1, part] * alpha + jnp.sum(p, axis=0, keepdims=True)
            m_ref[:1, part] = m_new
            pv = lax.dot_general(k[:, :LATENT], p.astype(jnp.bfloat16), (((0,), (0,)), ((), ())), preferred_element_type=jnp.float32)
            acc_ref[:, part] = acc_ref[:, part] * alpha + pv
        return carry

    lax.fori_loop(0, cache_chunks + new_chunks, step, 0)

    for h in range(heads):
        u, at = divmod(h, per)
        part = slice(h * tok, (h + 1) * tok)
        mixed = (acc_ref[:, part] * (1.0 / l_ref[:1, part])).astype(jnp.bfloat16)
        out = lax.dot_general(
            mixed,
            weight(LATENT, LATENT, h),
            (((0,), (0,)), ((), ())),
            preferred_element_type=jnp.float32,
        ).astype(jnp.bfloat16)
        o_own[slot + u, :, at * VH : (at + 1) * VH] = out[:half]
        o_far[u, :, at * VH : (at + 1) * VH] = out[half:]


def attend(meta, queries, q_far, weights, keys, cos, sin, out_own, out_far, first, slot, slots, cache_all):
    n_w = len(weights)
    half = queries.shape[0]
    width = q_far.shape[2]
    heads = width // (NOPE + ROPE)
    rows = n_w * heads * 2 * half
    total = keys.shape[0]
    vmem = pl.BlockSpec(memory_space=pltpu.VMEM)
    operands = [*weights, queries, q_far, keys, cos, sin]
    in_specs = [vmem] * len(operands)
    aliases = {}
    for value, position in ((out_own, 0), (out_far, 1)):
        if value is not None:
            aliases[1 + len(operands)] = position
            operands.append(value)
            in_specs.append(pl.BlockSpec(memory_space=pl.ANY) if position else vmem)
    return pl.pallas_call(
        functools.partial(attend_kernel, cache_all, n_w, len(aliases), first, slot),
        out_shape=(
            jax.ShapeDtypeStruct((slots, half, heads * VH), jnp.bfloat16),
            jax.ShapeDtypeStruct((slots, half, heads * VH), jnp.bfloat16),
        ),
        grid_spec=pltpu.PrefetchScalarGridSpec(
            num_scalar_prefetch=1,
            grid=(1,),
            in_specs=in_specs,
            out_specs=(
                vmem,
                pl.BlockSpec((n_w, half, heads * VH), lambda u, m: (slot // n_w, 0, 0)),
            ),
            scratch_shapes=[
                pltpu.VMEM((LATENT + 2 * ROPE, rows), jnp.bfloat16),
                pltpu.VMEM((8, rows), jnp.float32),
                pltpu.VMEM((8, rows), jnp.float32),
                pltpu.VMEM((LATENT, rows), jnp.float32),
            ],
        ),
        input_output_aliases=aliases,
        compiler_params=pltpu.CompilerParams(
            dimension_semantics=("arbitrary",), vmem_limit_bytes=12 * 1024 * 1024,
        ),
        cost_estimate=pl.CostEstimate(
            flops=rows * total * 2 * 1280,
            bytes_accessed=12_000_000,
            transcendentals=rows * total,
        ),
    )(meta, *operands)


def choose_kernel(first_ref, one_ref, two_ref, out_ref):
    @pl.when(first_ref[0] != 0)
    def _():
        out_ref[...] = one_ref[...]

    @pl.when(first_ref[0] == 0)
    def _():
        out_ref[...] = two_ref[...]


def choose(first, one, two):
    vmem = pl.BlockSpec(memory_space=pltpu.VMEM)
    return pl.pallas_call(
        choose_kernel,
        out_shape=jax.ShapeDtypeStruct(one.shape, one.dtype),
        in_specs=[pl.BlockSpec(memory_space=pltpu.SMEM), vmem, vmem],
        out_specs=vmem,
        cost_estimate=pl.CostEstimate(flops=2_000_000, bytes_accessed=6 * one.size, transcendentals=0),
        compiler_params=pltpu.CompilerParams(vmem_limit_bytes=8 * 1024 * 1024),
        name="choose",
    )(first.astype(jnp.int32).reshape(1), one, two)


def merge_kernel(starts, meta_ref, far_cols_ref, *refs):
    packed, out_ref, sem = refs[: 2 * len(starts)], refs[-2], refs[-1]
    copies = []
    for i, ref in enumerate(packed):
        width = ref.shape[2]
        for u in range(ref.shape[0]):
            unit = starts[i // 2] + u
            owner = far_cols_ref[unit] if i % 2 else meta_ref[4 + unit]
            column = pl.multiple_of(owner * width, width)
            copies.append(
                pltpu.make_async_copy(
                    ref.at[u], out_ref.at[:, pl.ds(column, width)], sem.at[len(copies)]
                )
            )
    for copy in copies:
        copy.start()
    for copy in copies:
        copy.wait()


def merge(meta, far_cols, landed, out, columns):
    starts = tuple(start for start, _, _ in landed)
    packed = [value for _, *values in landed for value in values]
    vmem = pl.BlockSpec(memory_space=pltpu.VMEM)
    smem = pl.BlockSpec(memory_space=pltpu.SMEM)
    chain = [] if out is None else [out]
    return pl.pallas_call(
        functools.partial(merge_kernel, starts),
        out_shape=jax.ShapeDtypeStruct((packed[0].shape[1], columns), packed[0].dtype),
        in_specs=[smem, smem] + [vmem] * len(packed) + [pl.BlockSpec(memory_space=pl.ANY)] * len(chain),
        out_specs=pl.BlockSpec(memory_space=pl.ANY),
        scratch_shapes=[pltpu.SemaphoreType.DMA((sum(v.shape[0] for v in packed),))],
        input_output_aliases={2 + len(packed): 0} if chain else {},
        cost_estimate=pl.CostEstimate(
            flops=5_000_000, bytes_accessed=4 * sum(v.size for v in packed), transcendentals=0
        ),
        compiler_params=pltpu.CompilerParams(vmem_limit_bytes=6 * 1024 * 1024),
        name="merge",
    )(meta, far_cols, *packed, *chain)


def local(queries, kv_new, kv_cache, kv_gain, w_key, w_value, prefix_len):
    gx, gy, chips = lax.axis_size("gx"), lax.axis_size("gy"), lax.axis_size("sz")
    x, y, here, core = (lax.axis_index(a) for a in ("gx", "gy", "sz", "sc"))
    tok_dev = queries.shape[0]
    cache_dev = kv_cache.shape[0]
    heads_dev = w_key.shape[1] // NOPE
    width = heads_dev * (NOPE + ROPE)
    cache_all = 2 * chips * cache_dev
    far_steps = chips // 2
    stretch_start = prefix_len[0]

    swap = [(0, 1), (1, 0)]
    ring = []
    for i in range(chips):
        ring += [(2 * i, 2 * ((i + 1) % chips)), (2 * i + 1, 2 * ((i - 1) % chips) + 1)]
    pairs = []
    for i in range(gx):
        for j in range(gy):
            at = (i * gy + j) * 2
            pairs += [(at, ((i ^ 1) * gy + j) * 2), (at + 1, (i * gy + (j ^ 1)) * 2 + 1)]

    def across(v):
        return lax.ppermute(v, "sc", swap)

    def along(v):
        return lax.ppermute(v, ("sz", "sc"), ring)

    def beside(v):
        return lax.ppermute(v, ("gx", "gy", "sc"), pairs)

    def owners(side):
        bit = jnp.where(side == 0, x % 2, y % 2)
        turn = jnp.where(side == 0, chips - 1, 1)
        units = [2 * here + side]
        for k in range(1, far_steps):
            chip = lax.rem(here + k * turn, chips)
            units += [2 * chip + bit, 2 * chip + 1 - bit]
        units.append(2 * lax.rem(here + far_steps, chips) + side)
        return jnp.stack(units).astype(jnp.int32)

    seat = 2 * here + core
    offsets = jnp.arange(tok_dev, dtype=jnp.int32)
    positions = stretch_start + seat * tok_dev + offsets
    phases = phases_for(positions, ROPE)
    raw_latent = kv_new[:, :LATENT].astype(jnp.float32)
    inv_rms = lax.rsqrt(jnp.mean(raw_latent * raw_latent, axis=1, keepdims=True) + EPS)
    latent_new = (raw_latent * inv_rms * kv_gain[None, :]).astype(jnp.bfloat16)
    rope_new = rotate(kv_new[:, LATENT:].astype(jnp.float32), phases).astype(jnp.bfloat16)
    mine = jnp.concatenate([kv_cache, jnp.concatenate([latent_new, rope_new], 1)], 0)
    own_cols, far_cols = owners(core), owners(1 - core)
    block = jnp.concatenate([mine, across(mine)], 0)
    block, w_key, w_value, far_cols = lax.optimization_barrier((block, w_key, w_value, far_cols))
    blocks, fars = [block], []
    for k in range(1, far_steps + 1):
        blocks.append(along(blocks[-1]))
        if k < far_steps:
            fars.append(across(blocks[k]))
    keys = build_keys(
        jnp.stack([here, core]).astype(jnp.int32), blocks + fars, chips, cache_dev, tok_dev
    )
    packed = pack_queries(queries, far_cols, width)
    q_far = across(packed)
    w_mine = jnp.concatenate([w_key, w_value], 0)
    bit = jnp.where(core == 0, x % 2, y % 2)
    far_mine = across(w_mine)
    travel = choose(bit == core, w_mine, far_mine)

    both = jnp.concatenate([positions, stretch_start + (2 * here + 1 - core) * tok_dev + offsets])
    turns = phases_for(both, ROPE)
    cos = jnp.concatenate([jnp.cos(turns)] * 2, 1)
    sin = jnp.concatenate([-jnp.sin(turns), jnp.sin(turns)], 1)
    meta = jnp.concatenate(
        [
            jnp.stack(
                [
                    stretch_start,
                    seat * tok_dev,
                    (2 * here + 1 - core) * tok_dev,
                    (here + 1) * 2 * tok_dev,
                ]
            ).astype(jnp.int32),
            own_cols,
        ]
    )
    near = along(travel)
    aside = w_mine
    result, first = None, 0
    columns = 2 * chips * heads_dev * VH
    landed = []
    cuts = (0, far_steps // 2, far_steps, far_steps + 1)
    for begin, end in zip(cuts, cuts[1:]):
        sizes = [2 if k < far_steps - 1 else 1 for k in range(begin, end)]
        out_own, out_far, slot = None, None, 0
        for k in range(begin, end):
            if k < far_steps - 1:
                weights = (aside, near)
                aside = beside(near)
                if k < far_steps - 2:
                    near = along(near)
            elif k == far_steps - 1:
                weights = (aside,)
                near = along(choose(bit == core, near, aside))
            else:
                weights = (near,)
            out_own, out_far = attend(
                meta, queries, q_far, weights, keys, cos, sin,
                out_own, out_far, first, slot, sum(sizes), cache_all,
            )
            first += len(weights)
            slot += len(weights)
            if landed and k == begin and end <= far_steps:
                result = merge(meta, far_cols, landed, result, columns)
                landed = []
        landed.append((first - slot, out_own, across(out_far)))
    return merge(meta, far_cols, landed, result, columns)


def solution(mesh):
    groups, seq = mesh.shape["groups"], mesh.shape["seq"]
    gy = math.isqrt(groups)
    torus = Mesh(
        mesh.devices.reshape(groups // gy, gy, seq // 2, 2), ("gx", "gy", "sz", "sc")
    )
    every = ("gx", "gy", "sz", "sc")
    line = ("sz", "sc")
    placed = (
        P(every, None),
        P(every, None),
        P(every, None),
        P(),
        P(None, line),
        P(None, line),
        P(("gx", "gy")),
    )
    return jax.shard_map(
        local, mesh=torus, in_specs=placed, out_specs=P(every, None), check_vma=False
    )
```

```python
import functools
import math

import jax
import jax.numpy as jnp
from jax import lax
from jax.experimental import pallas as pl
from jax.experimental.pallas import tpu as pltpu
from jax.sharding import Mesh
from jax.sharding import PartitionSpec as P

NOPE = 128
ROPE = 64
LATENT = 512
VH = 128
EPS = 1e-06
CHUNK = 1024
PART = 512
NEG = -1e30


def phases_for(positions, rope_width):
    half_width = rope_width // 2
    inverse = 10000.0 ** (-(jnp.arange(half_width, dtype=jnp.float32) * 2.0) / rope_width)
    return positions.astype(jnp.float32)[:, None] * inverse[None, :]


def rotate(values, phases):
    half_width = values.shape[-1] // 2
    front_half = values[..., :half_width]
    back_half = values[..., half_width:]
    cosine = jnp.cos(phases)
    sine_part = jnp.sin(phases)
    return jnp.concatenate(
        [front_half * cosine - back_half * sine_part, back_half * cosine + front_half * sine_part],
        -1,
    )


def pack_kernel(cols_ref, q_ref, o_ref, sem):
    width = o_ref.shape[2]
    copies = [
        pltpu.make_async_copy(
            q_ref.at[:, pl.ds(pl.multiple_of(cols_ref[u] * width, width), width)],
            o_ref.at[u],
            sem.at[u],
        )
        for u in range(o_ref.shape[0])
    ]
    for copy in copies:
        copy.start()
    for copy in copies:
        copy.wait()


def pack_queries(queries, cols, width):
    units = cols.shape[0]
    rows = queries.shape[0]
    return pl.pallas_call(
        pack_kernel,
        out_shape=jax.ShapeDtypeStruct((units, rows, width), queries.dtype),
        in_specs=[pl.BlockSpec(memory_space=pltpu.SMEM), pl.BlockSpec(memory_space=pl.ANY)],
        out_specs=pl.BlockSpec(memory_space=pltpu.VMEM),
        scratch_shapes=[pltpu.SemaphoreType.DMA((units,))],
        cost_estimate=pl.CostEstimate(
            flops=5_000_000, bytes_accessed=4 * units * rows * width, transcendentals=0
        ),
        compiler_params=pltpu.CompilerParams(vmem_limit_bytes=4 * 1024 * 1024),
        name="pack",
    )(cols, queries)


def keys_kernel(chips, cache_dev, tok_dev, meta_ref, *refs):
    *ins, far_ref, out_ref = refs
    here, core = meta_ref[0], meta_ref[1]
    cache_all = chips * 2 * cache_dev
    rows = cache_dev + tok_dev
    out_ref[:, LATENT + ROPE :] = jnp.zeros_like(out_ref[:, LATENT + ROPE :])

    def place(block, chip, first_core):
        for part in range(2):
            seat = 2 * chip + (first_core if part == 0 else 1 - first_core)
            at = pl.multiple_of(seat * cache_dev, cache_dev)
            out_ref[pl.ds(at, cache_dev), : LATENT + ROPE] = block[
                part * rows : part * rows + cache_dev
            ]
            at = pl.multiple_of(cache_all + seat * tok_dev, tok_dev)
            out_ref[pl.ds(at, tok_dev), : LATENT + ROPE] = block[
                part * rows + cache_dev : (part + 1) * rows
            ]

    sign = jnp.where(core == 0, chips - 1, 1)
    for k, ref in enumerate(ins):
        place(ref[...], lax.rem(here + k * sign, chips), core)
    for k in range(far_ref.shape[0]):
        place(far_ref[k], lax.rem(here + (k + 1) * (chips - sign), chips), 1 - core)


def stack_kernel(*refs):
    for k, ref in enumerate(refs[:-1]):
        refs[-1][k] = ref[...]


def stack_blocks(blocks):
    vmem = pl.BlockSpec(memory_space=pltpu.VMEM)
    return pl.pallas_call(
        stack_kernel,
        out_shape=jax.ShapeDtypeStruct((len(blocks), *blocks[0].shape), blocks[0].dtype),
        in_specs=[vmem] * len(blocks),
        out_specs=vmem,
        cost_estimate=pl.CostEstimate(
            flops=2_000_000, bytes_accessed=4 * len(blocks) * blocks[0].size, transcendentals=0
        ),
        compiler_params=pltpu.CompilerParams(vmem_limit_bytes=8 * 1024 * 1024),
        name="stack",
    )(*blocks)


def build_keys(meta, ins, chips, cache_dev, tok_dev):
    total = chips * 2 * (cache_dev + tok_dev)
    width = LATENT + 2 * ROPE
    vmem = pl.BlockSpec(memory_space=pltpu.VMEM)
    return pl.pallas_call(
        functools.partial(keys_kernel, chips, cache_dev, tok_dev),
        out_shape=jax.ShapeDtypeStruct((total, width), jnp.bfloat16),
        in_specs=[pl.BlockSpec(memory_space=pltpu.SMEM)] + [vmem] * len(ins),
        out_specs=vmem,
        cost_estimate=pl.CostEstimate(
            flops=5_000_000, bytes_accessed=4 * total * width, transcendentals=0
        ),
        compiler_params=pltpu.CompilerParams(vmem_limit_bytes=16 * 1024 * 1024),
        name="keys",
    )(meta, *ins)


def attend_kernel(cache_all, n_w, chain, first, slot, meta_ref, *refs):
    w_refs = refs[:n_w]
    q_own, q_far, keys_ref, cos_ref, sin_ref = refs[n_w : 5 + n_w]
    o_own, o_far, qa_ref, m_ref, l_ref, acc_ref = refs[5 + n_w + chain :]
    half, width = q_far.shape[1:]
    tok = 2 * half
    per = width // (NOPE + ROPE)
    heads = n_w * per
    rows = heads * tok

    live_cache, first_own, first_far = meta_ref[0], meta_ref[1], meta_ref[2]
    new_count = meta_ref[3]
    scale = 1.0 / math.sqrt(NOPE + ROPE) * math.log2(math.e)

    def weight(start, count, h):
        u, at = divmod(h, per)
        return w_refs[u][start : start + count, at * NOPE : (at + 1) * NOPE]

    for h in range(heads):
        u, at = divmod(h, per)
        at = at * (NOPE + ROPE)
        if at == 0:
            column = pl.multiple_of(meta_ref[4 + first + u] * width, width)
            unit = jnp.concatenate([q_own[:, pl.ds(column, width)], q_far[first + u]], 0)
        block = unit[:, at : at + NOPE + ROPE]
        absorbed = lax.dot_general(
            weight(0, LATENT, h),
            block[:, :NOPE],
            (((1,), (1,)), ((), ())),
            preferred_element_type=jnp.float32,
        )
        rot = block[:, NOPE:].astype(jnp.float32)
        turned = jnp.concatenate([rot[:, ROPE // 2 :], rot[:, : ROPE // 2]], 1)
        rot = (rot * cos_ref[...] + turned * sin_ref[...]) * scale
        rot = jnp.concatenate([rot, jnp.zeros_like(rot)], 1).T
        qa_ref[:LATENT, h * tok : (h + 1) * tok] = (absorbed * scale).astype(jnp.bfloat16)
        qa_ref[LATENT:, h * tok : (h + 1) * tok] = rot.astype(jnp.bfloat16)

    m_ref[...] = jnp.full_like(m_ref, NEG)
    l_ref[...] = jnp.zeros_like(l_ref)
    acc_ref[...] = jnp.zeros_like(acc_ref)
    cache_chunks = (live_cache + CHUNK - 1) // CHUNK
    new_chunks = (new_count + CHUNK - 1) // CHUNK
    key = lax.broadcasted_iota(jnp.int32, (CHUNK, tok), 0)
    row = lax.broadcasted_iota(jnp.int32, (1, tok), 1)
    last = jnp.where(row < half, first_own + row, first_far + row - half) + (cache_all + 1)

    def step(t, carry):
        index = jnp.where(t < cache_chunks, t, t - cache_chunks + cache_all // CHUNK)
        base = pl.multiple_of(index * CHUNK, CHUNK)
        k = keys_ref[pl.ds(base, CHUNK), :]
        limit = jnp.where(t < cache_chunks, live_cache, last) - base
        mask = key < limit
        parts = [slice(g * PART, (g + 1) * PART) for g in range(rows // PART)]
        scores = [jnp.dot(k, qa_ref[:, part], preferred_element_type=jnp.float32) for part in parts]
        for part, s in zip(parts, scores):
            s = jnp.concatenate(
                [jnp.where(mask, s[:, i * tok : (i + 1) * tok], NEG) for i in range(PART // tok)], 1
            )
            m_old = m_ref[:1, part]
            m_new = jnp.maximum(m_old, jnp.max(s, axis=0, keepdims=True))
            alpha = jnp.exp2(m_old - m_new)
            p = jnp.exp2(s - m_new)
            l_ref[:1, part] = l_ref[:1, part] * alpha + jnp.sum(p, axis=0, keepdims=True)
            m_ref[:1, part] = m_new
            pv = lax.dot_general(k[:, :LATENT], p.astype(jnp.bfloat16), (((0,), (0,)), ((), ())), preferred_element_type=jnp.float32)
            acc_ref[:, part] = acc_ref[:, part] * alpha + pv
        return carry

    lax.fori_loop(0, cache_chunks + new_chunks, step, 0)

    for h in range(heads):
        u, at = divmod(h, per)
        part = slice(h * tok, (h + 1) * tok)
        mixed = (acc_ref[:, part] * (1.0 / l_ref[:1, part])).astype(jnp.bfloat16)
        out = lax.dot_general(
            mixed,
            weight(LATENT, LATENT, h),
            (((0,), (0,)), ((), ())),
            preferred_element_type=jnp.float32,
        ).astype(jnp.bfloat16)
        o_own[slot + u, :, at * VH : (at + 1) * VH] = out[:half]
        o_far[u, :, at * VH : (at + 1) * VH] = out[half:]


def attend(meta, queries, q_far, weights, keys, cos, sin, out_own, out_far, first, slot, slots, cache_all):
    n_w = len(weights)
    half = queries.shape[0]
    width = q_far.shape[2]
    heads = width // (NOPE + ROPE)
    rows = n_w * heads * 2 * half
    total = keys.shape[0]
    vmem = pl.BlockSpec(memory_space=pltpu.VMEM)
    operands = [*weights, queries, q_far, keys, cos, sin]
    in_specs = [vmem] * len(operands)
    aliases = {}
    for value, position in ((out_own, 0), (out_far, 1)):
        if value is not None:
            aliases[1 + len(operands)] = position
            operands.append(value)
            in_specs.append(pl.BlockSpec(memory_space=pl.ANY) if position else vmem)
    return pl.pallas_call(
        functools.partial(attend_kernel, cache_all, n_w, len(aliases), first, slot),
        out_shape=(
            jax.ShapeDtypeStruct((slots, half, heads * VH), jnp.bfloat16),
            jax.ShapeDtypeStruct((slots, half, heads * VH), jnp.bfloat16),
        ),
        grid_spec=pltpu.PrefetchScalarGridSpec(
            num_scalar_prefetch=1,
            grid=(1,),
            in_specs=in_specs,
            out_specs=(
                vmem,
                pl.BlockSpec((n_w, half, heads * VH), lambda u, m: (slot // n_w, 0, 0)),
            ),
            scratch_shapes=[
                pltpu.VMEM((LATENT + 2 * ROPE, rows), jnp.bfloat16),
                pltpu.VMEM((8, rows), jnp.float32),
                pltpu.VMEM((8, rows), jnp.float32),
                pltpu.VMEM((LATENT, rows), jnp.float32),
            ],
        ),
        input_output_aliases=aliases,
        compiler_params=pltpu.CompilerParams(
            dimension_semantics=("arbitrary",), vmem_limit_bytes=12 * 1024 * 1024,
        ),
        cost_estimate=pl.CostEstimate(
            flops=rows * total * 2 * 1280,
            bytes_accessed=12_000_000,
            transcendentals=rows * total,
        ),
    )(meta, *operands)


def choose_kernel(first_ref, one_ref, two_ref, out_ref):
    @pl.when(first_ref[0] != 0)
    def _():
        out_ref[...] = one_ref[...]

    @pl.when(first_ref[0] == 0)
    def _():
        out_ref[...] = two_ref[...]


def choose(first, one, two):
    vmem = pl.BlockSpec(memory_space=pltpu.VMEM)
    return pl.pallas_call(
        choose_kernel,
        out_shape=jax.ShapeDtypeStruct(one.shape, one.dtype),
        in_specs=[pl.BlockSpec(memory_space=pltpu.SMEM), vmem, vmem],
        out_specs=vmem,
        cost_estimate=pl.CostEstimate(flops=2_000_000, bytes_accessed=6 * one.size, transcendentals=0),
        compiler_params=pltpu.CompilerParams(vmem_limit_bytes=8 * 1024 * 1024),
        name="choose",
    )(first.astype(jnp.int32).reshape(1), one, two)


def merge_kernel(starts, meta_ref, far_cols_ref, *refs):
    packed, out_ref, sem = refs[: 2 * len(starts)], refs[-2], refs[-1]
    copies = []
    for i, ref in enumerate(packed):
        width = ref.shape[2]
        for u in range(ref.shape[0]):
            unit = starts[i // 2] + u
            owner = far_cols_ref[unit] if i % 2 else meta_ref[4 + unit]
            column = pl.multiple_of(owner * width, width)
            copies.append(
                pltpu.make_async_copy(
                    ref.at[u], out_ref.at[:, pl.ds(column, width)], sem.at[len(copies)]
                )
            )
    for copy in copies:
        copy.start()
    for copy in copies:
        copy.wait()


def merge(meta, far_cols, landed, out, columns):
    starts = tuple(start for start, _, _ in landed)
    packed = [value for _, *values in landed for value in values]
    vmem = pl.BlockSpec(memory_space=pltpu.VMEM)
    smem = pl.BlockSpec(memory_space=pltpu.SMEM)
    chain = [] if out is None else [out]
    return pl.pallas_call(
        functools.partial(merge_kernel, starts),
        out_shape=jax.ShapeDtypeStruct((packed[0].shape[1], columns), packed[0].dtype),
        in_specs=[smem, smem] + [vmem] * len(packed) + [pl.BlockSpec(memory_space=pl.ANY)] * len(chain),
        out_specs=pl.BlockSpec(memory_space=pl.ANY),
        scratch_shapes=[pltpu.SemaphoreType.DMA((sum(v.shape[0] for v in packed),))],
        input_output_aliases={2 + len(packed): 0} if chain else {},
        cost_estimate=pl.CostEstimate(
            flops=5_000_000, bytes_accessed=4 * sum(v.size for v in packed), transcendentals=0
        ),
        compiler_params=pltpu.CompilerParams(vmem_limit_bytes=6 * 1024 * 1024),
        name="merge",
    )(meta, far_cols, *packed, *chain)


def local(queries, kv_new, kv_cache, kv_gain, w_key, w_value, prefix_len):
    gx, gy, chips = lax.axis_size("gx"), lax.axis_size("gy"), lax.axis_size("sz")
    x, y, here, core = (lax.axis_index(a) for a in ("gx", "gy", "sz", "sc"))
    tok_dev = queries.shape[0]
    cache_dev = kv_cache.shape[0]
    heads_dev = w_key.shape[1] // NOPE
    width = heads_dev * (NOPE + ROPE)
    cache_all = 2 * chips * cache_dev
    far_steps = chips // 2
    stretch_start = prefix_len[0]

    swap = [(0, 1), (1, 0)]
    ring = []
    for i in range(chips):
        ring += [(2 * i, 2 * ((i + 1) % chips)), (2 * i + 1, 2 * ((i - 1) % chips) + 1)]
    pairs = []
    for i in range(gx):
        for j in range(gy):
            at = (i * gy + j) * 2
            pairs += [(at, ((i ^ 1) * gy + j) * 2), (at + 1, (i * gy + (j ^ 1)) * 2 + 1)]

    def across(v):
        return lax.ppermute(v, "sc", swap)

    def along(v):
        return lax.ppermute(v, ("sz", "sc"), ring)

    def beside(v):
        return lax.ppermute(v, ("gx", "gy", "sc"), pairs)

    def owners(side):
        bit = jnp.where(side == 0, x % 2, y % 2)
        turn = jnp.where(side == 0, chips - 1, 1)
        units = [2 * here + side]
        for k in range(1, far_steps):
            chip = lax.rem(here + k * turn, chips)
            units += [2 * chip + bit, 2 * chip + 1 - bit]
        units.append(2 * lax.rem(here + far_steps, chips) + side)
        return jnp.stack(units).astype(jnp.int32)

    seat = 2 * here + core
    offsets = jnp.arange(tok_dev, dtype=jnp.int32)
    positions = stretch_start + seat * tok_dev + offsets
    phases = phases_for(positions, ROPE)
    raw_latent = kv_new[:, :LATENT].astype(jnp.float32)
    inv_rms = lax.rsqrt(jnp.mean(raw_latent * raw_latent, axis=1, keepdims=True) + EPS)
    latent_new = (raw_latent * inv_rms * kv_gain[None, :]).astype(jnp.bfloat16)
    rope_new = rotate(kv_new[:, LATENT:].astype(jnp.float32), phases).astype(jnp.bfloat16)
    mine = jnp.concatenate([kv_cache, jnp.concatenate([latent_new, rope_new], 1)], 0)
    own_cols, far_cols = owners(core), owners(1 - core)
    block = jnp.concatenate([mine, across(mine)], 0)
    block, w_key, w_value, far_cols = lax.optimization_barrier((block, w_key, w_value, far_cols))
    blocks = [block]
    for _ in range(1, far_steps + 1):
        blocks.append(along(blocks[-1]))
    stacked = stack_blocks(blocks[1:far_steps])
    far = across(stacked)
    keys = build_keys(
        jnp.stack([here, core]).astype(jnp.int32), blocks + [far], chips, cache_dev, tok_dev
    )
    packed = pack_queries(queries, far_cols, width)
    q_far = across(packed)
    w_mine = jnp.concatenate([w_key, w_value], 0)
    bit = jnp.where(core == 0, x % 2, y % 2)
    far_mine = across(w_mine)
    travel = choose(bit == core, w_mine, far_mine)

    both = jnp.concatenate([positions, stretch_start + (2 * here + 1 - core) * tok_dev + offsets])
    turns = phases_for(both, ROPE)
    cos = jnp.concatenate([jnp.cos(turns)] * 2, 1)
    sin = jnp.concatenate([-jnp.sin(turns), jnp.sin(turns)], 1)
    meta = jnp.concatenate(
        [
            jnp.stack(
                [
                    stretch_start,
                    seat * tok_dev,
                    (2 * here + 1 - core) * tok_dev,
                    (here + 1) * 2 * tok_dev,
                ]
            ).astype(jnp.int32),
            own_cols,
        ]
    )
    near = along(travel)
    aside = w_mine
    result, first = None, 0
    columns = 2 * chips * heads_dev * VH
    landed = []
    cuts = (0, far_steps // 2, far_steps, far_steps + 1)
    for begin, end in zip(cuts, cuts[1:]):
        sizes = [2 if k < far_steps - 1 else 1 for k in range(begin, end)]
        out_own, out_far, slot = None, None, 0
        for k in range(begin, end):
            if k < far_steps - 1:
                weights = (aside, near)
                aside = beside(near)
                if k < far_steps - 2:
                    near = along(near)
            elif k == far_steps - 1:
                weights = (aside,)
                near = along(choose(bit == core, near, aside))
            else:
                weights = (near,)
            out_own, out_far = attend(
                meta, queries, q_far, weights, keys, cos, sin,
                out_own, out_far, first, slot, sum(sizes), cache_all,
            )
            first += len(weights)
            slot += len(weights)
            if landed and k == begin and end <= far_steps:
                result = merge(meta, far_cols, landed, result, columns)
                landed = []
        landed.append((first - slot, out_own, across(out_far)))
    return merge(meta, far_cols, landed, result, columns)


def solution(mesh):
    groups, seq = mesh.shape["groups"], mesh.shape["seq"]
    gy = math.isqrt(groups)
    torus = Mesh(
        mesh.devices.reshape(groups // gy, gy, seq // 2, 2), ("gx", "gy", "sz", "sc")
    )
    every = ("gx", "gy", "sz", "sc")
    line = ("sz", "sc")
    placed = (
        P(every, None),
        P(every, None),
        P(every, None),
        P(),
        P(None, line),
        P(None, line),
        P(("gx", "gy")),
    )
    return jax.shard_map(
        local, mesh=torus, in_specs=placed, out_specs=P(every, None), check_vma=False
    )
```
